1024 devices in a mesh: grp: 32 (over y_hi, z), shell: 32 (over x, y_lo, core).
Axes of the slice: x: 4, y: 8 (y_hi: 2, y_lo: 4; y = y_hi * 4 + y_lo), z: 16, core: 2. Of those that a mesh axis runs over, the one named last changes fastest.
Arguments:
- vectors: bfloat16 [32, 32, 384, 256], P('grp', 'shell'), may hold values from -6 to 6
- local_block: bfloat16 [32, 32, 384, 384], P('grp', 'shell'), may hold values from -0.3125 to 0.3125
- pair_blocks: bfloat16 [32, 32, 4, 384, 384], P('grp', 'shell'), may hold values from -0.3125 to 0.3125
- pair_masks: int32 [32, 32, 4, 3, 3], P('grp', 'shell'), may hold values 0 or 1
- shell_block: bfloat16 [32, 32, 384, 384], P('grp', 'shell'), may hold values from -0.3125 to 0.3125
- shell_mask: int32 [32, 32, 3, 3], P('grp', 'shell'), may hold values 0 or 1
- matchings: int32 [4, 32], replicated, may hold values from 0 to 31, as said below
Outputs:
- filtered: bfloat16 [32, 32, 384, 256], P('grp', 'shell')
The draws below stay inside these ranges and needn't reach their ends.
Inputs may be any that keep to these rules, and one draw needn't show every extreme that they name: Row m of matchings maps every group g to g XOR 2**b_m, for 4 distinct binary digits b_m drawn from the seed.
All inputs are finite; a program needn't handle non-finite values. No bound on the sum of `pair_masks` or of `shell_mask` on one device may be relied on, other than what follows from the above.
Results may differ from the reference program's by a relative error of at most 0.0049.
Values may be sent and summed in bfloat16 or wider, within the bound.
No kernel may reach another device: no remote copies, remote signals or barrier semaphores. Data moves between devices by JAX's collectives and lax.ppermute only.
A program may use at most 32 MiB of HBM per device.

```python
import jax
import jax.numpy as jnp
from jax import lax

R = 384
NV = 256
DEG = 2
BLK = 128
RB = 3
MATCH = 4
N_GRP = 32
N_SHELL = 32


def draw_matchings(key, part):
    digits = N_GRP.bit_length() - 1
    own_key = jax.random.fold_in(key, 7919)
    scores = jax.random.randint(own_key, (digits,), 0, 1000003, dtype=jnp.int32)
    distinct = scores * digits + jnp.arange(digits, dtype=jnp.int32)
    order = jnp.argsort(distinct, stable=True).astype(jnp.int32)
    chosen_bits = order[:MATCH].astype(jnp.int32)
    groups = jnp.arange(N_GRP, dtype=jnp.int32)
    flips = jnp.left_shift(jnp.int32(1), chosen_bits)
    return jnp.bitwise_xor(groups[None, :], flips[:, None]).astype(jnp.int32)


def place_ends(values, key, low, high):
    extent = values.shape
    place = [jax.random.randint(jax.random.fold_in(key, axis), (), 0, extent[axis]) for axis in range(len(extent))]
    values = values.at[tuple(place)].set(low)
    longest = extent.index(max(extent))
    place[longest] = (place[longest] + 1) % extent[longest]
    return values.at[tuple(place)].set(high)


def block_scale(rng, extent, split, smallest, high):
    level, own = 1.0, jax.random.fold_in(rng, 6)
    for axis_at, shards_of in split:
        draws = jnp.exp(jax.random.uniform(jax.random.fold_in(own, axis_at), (shards_of,), jnp.float32, smallest / len(split), high / len(split)))
        level = level * jnp.repeat(draws, extent[axis_at] // shards_of).reshape([-1 if axis == axis_at else 1 for axis in range(len(extent))])
    return level


def centred(rng, extent, width, reach, pieces=(), held_as=jnp.bfloat16):
    values = width * jax.random.normal(rng, extent, jnp.float32)
    if pieces:
        values = values * block_scale(rng, extent, pieces, -0.22, 0.18)
    return jnp.clip(values, -reach, reach).astype(held_as)


def setup_inputs(seed: int = 0) -> dict:
    splits = jax.random.split(jax.random.key(seed), 8)
    return {
        "vectors": centred(splits[0], (N_GRP, N_SHELL, R, NV), 1.0, 6.0, ((0, 32), (1, 32))),
        "local_block": centred(splits[1], (N_GRP, N_SHELL, R, R), R ** -0.5, 0.3125, ((0, 32), (1, 32))),
        "pair_blocks": centred(splits[2], (N_GRP, N_SHELL, MATCH, R, R), R ** -0.5, 0.3125, ((0, 32), (1, 32))),
        "pair_masks": place_ends((jax.random.randint(splits[3], (N_GRP, N_SHELL, MATCH, RB, RB), 0, 4) < 3).astype(jnp.int32), jax.random.fold_in(splits[3], 1), 0, 1),
        "shell_block": centred(splits[4], (N_GRP, N_SHELL, R, R), R ** -0.5, 0.3125, ((0, 32), (1, 32))),
        "shell_mask": place_ends((jax.random.randint(splits[5], (N_GRP, N_SHELL, RB, RB), 0, 4) < 3).astype(jnp.int32), jax.random.fold_in(splits[5], 1), 0, 1),
        "matchings": draw_matchings(jax.random.fold_in(splits[7], 71), 0),
    }


spectrum_center = 1.0
spectrum_halfwidth = 6.0


def widen(mask):
    spread = jnp.repeat(jnp.repeat(mask, BLK, axis=-2), BLK, axis=-1)
    return spread.astype(jnp.bfloat16)


def apply_operator(vectors, local_block, pair_blocks, pair_masks, shell_block, shell_mask, matchings):
    groups = jnp.arange(N_GRP, dtype=jnp.int32)

    def partials(group):
        coupled_rows = (pair_blocks[group] * widen(pair_masks[group])).astype(jnp.float32)
        higher_rows = (shell_block[group] * widen(shell_mask[group])).astype(jnp.float32)
        resident_rows = vectors[group].astype(jnp.float32)
        returned = jnp.einsum("smrk,srv->smkv", coupled_rows, resident_rows).astype(jnp.bfloat16)
        lower_partner = jnp.einsum("yol,yox->ylx", higher_rows, resident_rows).astype(jnp.bfloat16)
        return returned, lower_partner

    returned, lower_partner = lax.map(partials, groups)

    def rows(group):
        coupled_rows = (pair_blocks[group] * widen(pair_masks[group])).astype(jnp.float32)
        higher_rows = (shell_block[group] * widen(shell_mask[group])).astype(jnp.float32)
        owned_rows = local_block[group].astype(jnp.float32)
        resident_rows = vectors[group].astype(jnp.float32)
        accumulated_rows = jnp.einsum("tjb,tbu->tju", owned_rows, resident_rows) + jnp.einsum("oqp,oqx->opx", owned_rows, resident_rows)
        for pairing_index in range(MATCH):
            partner = matchings[pairing_index, group]
            remote_rows = vectors[partner].astype(jnp.float32)
            accumulated_rows = accumulated_rows + jnp.einsum("tjb,tbu->tju", coupled_rows[:, pairing_index], remote_rows)
            accumulated_rows = accumulated_rows + returned[partner][:, pairing_index].astype(jnp.float32)
        zero_shell = jnp.zeros((1, R, NV), jnp.float32)
        higher_partner = jnp.concatenate([resident_rows[1:], zero_shell], axis=0)
        accumulated_rows = accumulated_rows + jnp.einsum("tjb,tbu->tju", higher_rows, higher_partner)
        lower_terms = lower_partner[group].astype(jnp.float32)
        accumulated_rows = accumulated_rows + jnp.concatenate([zero_shell, lower_terms[:-1]], axis=0)
        return accumulated_rows

    return lax.map(rows, groups)


def reference(vectors, local_block, pair_blocks, pair_masks, shell_block, shell_mask, matchings):
    def operate(current):
        return apply_operator(current, local_block, pair_blocks, pair_masks, shell_block, shell_mask, matchings)

    previous = vectors
    current = ((operate(vectors) - spectrum_center * vectors.astype(jnp.float32)) / spectrum_halfwidth).astype(jnp.bfloat16)
    for degree_step in range(1, DEG):
        image = operate(current)
        following = 2.0 * (image - spectrum_center * current.astype(jnp.float32)) / spectrum_halfwidth - previous.astype(jnp.float32)
        previous = current
        current = following.astype(jnp.bfloat16)
    return current
```

```python
import jax
import jax.numpy as jnp
from jax import lax
from jax.experimental import pallas as pl
from jax.experimental.pallas import tpu as pltpu
from jax.sharding import PartitionSpec as P

BLK = 128
RB = 3
R = 384
NV = 256
MATCH = 4
BITS = 5

spectrum_center = 1.0
spectrum_halfwidth = 6.0

VMEM = pl.BlockSpec(memory_space=pltpu.VMEM)
SMEM = pl.BlockSpec(memory_space=pltpu.SMEM)

ROWS = jax.ShapeDtypeStruct((R, NV), jnp.bfloat16)
PAIR = jax.ShapeDtypeStruct((2, R, NV), jnp.bfloat16)
TOTAL = jax.ShapeDtypeStruct((R, NV), jnp.float32)


def dot(a, b):
    return jnp.dot(a, b, preferred_element_type=jnp.float32)


def product(block, rows):
    return dot(block, rows).astype(jnp.bfloat16)


def masked(block, mask):
    return block * jnp.full((BLK, BLK), mask.astype(jnp.float32)).astype(jnp.bfloat16)


def prepare(group, matchings, pair_masks, shell_mask, v, pair, shell, local,
            pb, pt, cb, ct, lt, q3, q2, s1, s0, s4, up, total):
    g = group[0]
    rows = v[...]
    for b in (3, 2, 1, 0, 4):
        place, present = jnp.int32(0), jnp.int32(0)
        for m in range(MATCH):
            hit = (jnp.bitwise_xor(matchings[m, g], g) == 1 << b).astype(jnp.int32)
            place, present = place + hit * m, present + hit
        for i in range(RB):
            for j in range(RB):
                block = pair[place, i * BLK:(i + 1) * BLK, j * BLK:(j + 1) * BLK]
                block = masked(block, pair_masks[place * RB * RB + i * RB + j] * present)
                pb[b, i * BLK:(i + 1) * BLK, j * BLK:(j + 1) * BLK] = block
                pt[b, j * BLK:(j + 1) * BLK, i * BLK:(i + 1) * BLK] = block.T
        q = product(pt[b], rows)
        if b == 3:
            q3[...] = q
        elif b == 2:
            q2[...] = q
        else:
            send = {0: s0, 1: s1, 4: s4}[b]
            send[0] = rows
            send[1] = q
    for i in range(RB):
        for j in range(RB):
            block = masked(shell[i * BLK:(i + 1) * BLK, j * BLK:(j + 1) * BLK], shell_mask[i * RB + j])
            cb[i * BLK:(i + 1) * BLK, j * BLK:(j + 1) * BLK] = block
            ct[j * BLK:(j + 1) * BLK, i * BLK:(i + 1) * BLK] = block.T
    up[...] = product(ct[...], rows)
    lt[...] = local[...].T
    total[...] = dot(local[...], rows) + dot(lt[...], rows) - spectrum_center * rows.astype(jnp.float32)


def spread(v, pt, local, lt, ct, q2, s1, s0, s4, up, total):
    rows = v[...]
    q2[...] = product(pt[2], rows)
    for b, send in ((1, s1), (0, s0), (4, s4)):
        send[0] = rows
        send[1] = product(pt[b], rows)
    up[...] = product(ct[...], rows)
    total[...] = dot(local[...], rows) + dot(lt[...], rows) - spectrum_center * rows.astype(jnp.float32)


def collected(total, v2, v3, q, r1, r0, r4, higher, lower, pb, cb):
    image = total[...] + dot(pb[2], v2[...]) + dot(pb[3], v3[...]) + dot(cb[...], higher[...])
    for b, r in ((1, r1), (0, r0), (4, r4)):
        image = image + dot(pb[b], r[0]) + r[1].astype(jnp.float32)
    return image + q[...].astype(jnp.float32) + lower[...].astype(jnp.float32)


def first(total, v2, v3, q, r1, r0, r4, higher, lower, pb, cb, pt, out, q3):
    image = collected(total, v2, v3, q, r1, r0, r4, higher, lower, pb, cb)
    rows = (image / spectrum_halfwidth).astype(jnp.bfloat16)
    out[...] = rows
    q3[...] = product(pt[3], rows)


def second(total, v2, v3, q, r1, r0, r4, higher, lower, pb, cb, v, out):
    image = collected(total, v2, v3, q, r1, r0, r4, higher, lower, pb, cb)
    out[...] = (2.0 * image / spectrum_halfwidth - v[...].astype(jnp.float32)).astype(jnp.bfloat16)


def flops(products):
    return pl.CostEstimate(flops=products * 2 * R * R * NV, bytes_accessed=4 * R * R, transcendentals=0)


def call(body, outs, n_smem, n_vmem, products):
    return pl.pallas_call(
        body,
        out_shape=outs,
        in_specs=[SMEM] * n_smem + [VMEM] * n_vmem,
        out_specs=jax.tree.map(lambda _: VMEM, outs),
        cost_estimate=flops(products),
    )


def from_behind(block, distance):
    size = lax.axis_size("shell")
    return lax.ppermute(block, "shell", [(i - distance, i) for i in range(size) if 0 <= i - distance < size])


def from_partner(x, flip):
    return lax.ppermute(x, "grp", [(i, i ^ flip) for i in range(lax.axis_size("grp"))])


def exchange(v, q3, q2, s1, s0, s4, up):
    v2 = from_partner(v, 4)
    q3 = from_partner(q3, 12)
    r0 = from_partner(s0, 1)
    r1 = from_partner(s1, 2)
    r4 = from_partner(s4, 16)
    higher = from_behind(v, -1)
    lower = from_behind(up, 1)
    v3 = from_partner(v2, 12)
    q = from_partner((q2.astype(jnp.float32) + q3.astype(jnp.float32)).astype(jnp.bfloat16), 4)
    return v2, v3, q, r1, r0, r4, higher, lower


def on_device(vectors, local_block, pair_blocks, pair_masks, shell_block, shell_mask, matchings):
    v = vectors[0, 0]
    local = local_block[0, 0]
    group = lax.axis_index("grp").astype(jnp.int32).reshape(1)
    square = jax.ShapeDtypeStruct((R, R), jnp.bfloat16)
    stack = jax.ShapeDtypeStruct((BITS, R, R), jnp.bfloat16)
    pb, pt, cb, ct, lt, q3, q2, s1, s0, s4, up, total = call(
        prepare, [stack, stack, square, square, square, ROWS, ROWS, PAIR, PAIR, PAIR, ROWS, TOTAL], 4, 4, 8
    )(group, matchings, pair_masks.reshape(-1), shell_mask.reshape(-1), v, pair_blocks[0, 0], shell_block[0, 0], local)
    parts = exchange(v, q3, q2, s1, s0, s4, up)
    w, q3 = call(first, [ROWS, ROWS], 0, 12, 7)(total, *parts, pb, cb, pt)
    q2, s1, s0, s4, up, total = call(spread, [ROWS, PAIR, PAIR, PAIR, ROWS, TOTAL], 0, 5, 7)(w, pt, local, lt, ct)
    parts = exchange(w, q3, q2, s1, s0, s4, up)
    out = call(second, ROWS, 0, 12, 6)(total, *parts, pb, cb, v)
    return out[None, None]


def solution(mesh):
    in_specs = (
        P("grp", "shell", None, None),
        P("grp", "shell", None, None),
        P("grp", "shell", None, None, None),
        P("grp", "shell", None, None, None),
        P("grp", "shell", None, None),
        P("grp", "shell", None, None),
        P(),
    )
    out_specs = P("grp", "shell", None, None)
    return jax.shard_map(
        on_device, mesh=mesh, in_specs=in_specs, out_specs=out_specs, check_vma=False
    )
```

```python
import jax
import jax.numpy as jnp
from jax import lax
from jax.experimental import pallas as pl
from jax.experimental.pallas import tpu as pltpu
from jax.sharding import PartitionSpec as P

BLK = 128
RB = 3
R = 384
NV = 256
MATCH = 4


spectrum_center = 1.0
spectrum_halfwidth = 6.0

VMEM = pl.BlockSpec(memory_space=pltpu.VMEM)
SMEM = pl.BlockSpec(memory_space=pltpu.SMEM)

ROWS = pltpu.VMEM((R, NV), jnp.bfloat16)
PAIR = pltpu.VMEM((2, R, NV), jnp.bfloat16)
TOTAL = pltpu.VMEM((R, NV), jnp.float32)
SQUARE = pltpu.VMEM((R, R), jnp.bfloat16)


def dot(a, b):
    return jnp.dot(a, b, preferred_element_type=jnp.float32)


def product(block, rows):
    return dot(block, rows).astype(jnp.bfloat16)


def wide(x):
    return x.astype(jnp.float32)


def masked(block, mask):
    return block * jnp.full((BLK, BLK), wide(mask)).astype(jnp.bfloat16)


def sorted_block(b, matchings, pair_masks, pair, pb, pt, at):
    place, present = jnp.int32(0), jnp.int32(0)
    for m in range(MATCH):
        hit = (matchings[m, 0] == 1 << b).astype(jnp.int32)
        place, present = place + hit * m, present + hit
    for i in range(RB):
        for j in range(RB):
            rows, cols = slice(i * BLK, (i + 1) * BLK), slice(j * BLK, (j + 1) * BLK)
            block = masked(pair[place, rows, cols], pair_masks[0, i, j, 0, place] * present)
            pb[at, rows, cols] = block
            pt[at, cols, rows] = block.T


def prepare_far(matchings, pair_masks, v, pair, pb, pt, q3):
    sorted_block(3, matchings, pair_masks, pair, pb, pt, 0)
    q3[...] = product(pt[0], v[...])


def prepare_near(matchings, pair_masks, shell_mask, v, pair, shell, pb, pt, ct, cb, q2, s1, s0, s4, up):
    rows = v[...]
    for at, b in enumerate((4, 1, 0, 2)):
        sorted_block(b, matchings, pair_masks, pair, pb, pt, at)
        q = product(pt[at], rows)
        if b == 2:
            q2[...] = q
        else:
            send = {0: s0, 1: s1, 4: s4}[b]
            send[0] = rows
            send[1] = q
    for i in range(RB):
        for j in range(RB):
            rs, cs = slice(i * BLK, (i + 1) * BLK), slice(j * BLK, (j + 1) * BLK)
            block = masked(shell[rs, cs], shell_mask[0, i, 0, j])
            cb[rs, cs] = block
            ct[cs, rs] = block.T
    up[...] = product(ct[...], rows)


def spread(v, pt, ct, q2, s1, s0, s4, up):
    rows = v[...]
    for at, send in ((0, s4), (1, s1), (2, s0)):
        send[0] = rows
        send[1] = product(pt[at], rows)
    q2[...] = product(pt[3], rows)
    up[...] = product(ct[...], rows)


def resident(v, local, total):
    rows = v[...]
    total[...] = dot(local[...], rows) + dot(local[...].T, rows) - spectrum_center * wide(rows)


def gathered(total, v2, r1, r0, r4, higher, lower, pb, cb, image):
    image[...] = (total[...] + dot(pb[3], v2[...]) + dot(cb[...], higher[...]) + wide(lower[...])
                  + dot(pb[1], r1[0]) + wide(r1[1]) + dot(pb[2], r0[0]) + wide(r0[1])
                  + dot(pb[0], r4[0]) + wide(r4[1]))


def first(image, v3, q, pb, pt, out, q3):
    rows = ((image[...] + wide(q[...]) + dot(pb[0], v3[...])) / spectrum_halfwidth).astype(jnp.bfloat16)
    out[...] = rows
    q3[...] = product(pt[0], rows)


def second(image, v3, q, pb, v, out):
    total = image[...] + wide(q[...]) + dot(pb[0], v3[...])
    out[...] = (2.0 * total / spectrum_halfwidth - wide(v[...])).astype(jnp.bfloat16)


def added(a, b, out):
    out[...] = (wide(a[...]) + wide(b[...])).astype(jnp.bfloat16)


def call(body, outs, products, *args, n_smem=0):
    args = args[:n_smem] + tuple(pltpu.with_memory_space_constraint(x, pltpu.VMEM) for x in args[n_smem:])
    return pl.pallas_call(
        body,
        out_shape=outs,
        in_specs=[SMEM] * n_smem + [VMEM] * (len(args) - n_smem),
        out_specs=jax.tree.map(lambda _: VMEM, outs),
        compiler_params=pltpu.CompilerParams(vmem_limit_bytes=8 << 20),
        cost_estimate=pl.CostEstimate(flops=products * 2 * R * R * NV, bytes_accessed=4 * R * R, transcendentals=0),
    )(*args)


def from_behind(block, distance):
    size = lax.axis_size("shell")
    return lax.ppermute(block, "shell", [(i - distance, i) for i in range(size) if 0 <= i - distance < size])


def from_partner(x, flip):
    return lax.ppermute(x, "grp", [(i, i ^ flip) for i in range(lax.axis_size("grp"))])


def exchange(v, q3, near, local, cb, pb):
    v2 = from_partner(v, 4)
    q3 = from_partner(q3, 12)
    q2, s1, s0, s4, up = near()
    r4 = from_partner(s4, 16)
    r1 = from_partner(s1, 2)
    r0 = from_partner(s0, 1)
    higher = from_behind(v, -1)
    lower = from_behind(up, 1)
    v3 = from_partner(v2, 12)
    q = call(added, ROWS, 1, q2, q3)
    q = from_partner(q, 4)
    total = call(resident, TOTAL, 2, v, local)
    image = call(gathered, TOTAL, 5, total, v2, r1, r0, r4, higher, lower, pb(), cb())
    return image, v3, q


def on_device(vectors, local_block, pair_blocks, pair_masks, shell_block, shell_mask, matchings):
    v = vectors[0, 0]
    local = local_block[0, 0]
    pair = pair_blocks[0, 0]
    pair_masks = jnp.transpose(pair_masks, (0, 3, 4, 1, 2))
    shell_mask = jnp.transpose(shell_mask, (0, 2, 1, 3))
    one = pltpu.VMEM((1, R, R), jnp.bfloat16)
    four = pltpu.VMEM((4, R, R), jnp.bfloat16)
    pb3, pt3, q3 = call(prepare_far, [one, one, ROWS], 3, matchings, pair_masks, v, pair, n_smem=2)
    kept = {}

    def near():
        kept["pb"], kept["pt"], kept["ct"], kept["cb"], *sends = call(
            prepare_near, [four, four, SQUARE, SQUARE, ROWS, PAIR, PAIR, PAIR, ROWS], 12,
            matchings, pair_masks, shell_mask, v, pair, shell_block[0, 0], n_smem=3)
        return sends

    parts = exchange(v, q3, near, local, lambda: kept["cb"], lambda: kept["pb"])
    w, q3 = call(first, [ROWS, ROWS], 2, *parts, pb3, pt3)
    parts = exchange(
        w, q3,
        lambda: call(spread, [ROWS, PAIR, PAIR, PAIR, ROWS], 5, w, kept["pt"], kept["ct"]),
        local, lambda: kept["cb"], lambda: kept["pb"])
    out = call(second, ROWS, 1, *parts, pb3, v)
    return out[None, None]


def solution(mesh):
    in_specs = (
        P("grp", "shell", None, None),
        P("grp", "shell", None, None),
        P("grp", "shell", None, None, None),
        P("grp", "shell", None, None, None),
        P("grp", "shell", None, None),
        P("grp", "shell", None, None),
        P(),
    )
    out_specs = P("grp", "shell", None, None)
    return jax.shard_map(
        on_device, mesh=mesh, in_specs=in_specs, out_specs=out_specs, check_vma=False
    )
```
